512 devices in a mesh: gx: 8 (over z_lo, core), gy: 8 (over y), gz: 8 (over x, z_hi).
Axes of the slice: x: 4, y: 8, z: 8 (z_hi: 2, z_lo: 4; z = z_hi * 4 + z_lo), core: 2. Of those that a mesh axis runs over, the one named last changes fastest.
Arguments:
- right_side: float32 [131072, 2048], P(('gx', 'gy'), 'gz'), may hold values from -6 to 6
- send_order: int32 [64, 2048], P(('gx', 'gy')), may hold values from 0 to 2047, each once within a row
- recv_order: int32 [64, 2048], P(('gx', 'gy')), may hold values from 0 to 2047, each once within a row
- update_target: int32 [256, 2], P('gx'), may hold values from 0 to 63, as said below
- leaf_inv: float32 [256, 256, 256], P(('gx', 'gy'), 'gz'), may hold values from -0.375 to 0.375
- leaf_low: float32 [256, 256, 256], P(('gx', 'gy'), 'gz'), may hold values from -0.375 to 0.375
- parent_inv: float32 [128, 512, 512], P(('gx', 'gy'), 'gz'), may hold values from -0.25 to 0.25
Outputs:
- solution: float32 [131072, 2048], P(('gx', 'gy'), 'gz')
The draws below stay inside these ranges and needn't reach their ends.
Inputs may be any that keep to these rules, and one draw needn't show every extreme that they name: `update_target`: entries are 4 * parent + block, with parent counted among the 2 * 8 parents of the leaf's gx index and block below 4; a leaf's two entries name the same parent and two different blocks. Among the 4 leaves of one index of gx+gy, at most 1 name parents held by one index of gy (parent // 2), and exactly 1 do so for some index of gy.
All inputs are finite; a program needn't handle non-finite values.
Results may differ from the reference program's by a relative error of at most 0.000073.
Values sent between devices are 32-bit elements; how exact they have to be, the bound alone decides.
A program may use at most 64 MiB of HBM per device.

```python
import jax
import jax.numpy as jnp
from jax import lax

PIV = 256
BLK = 128
LEAF_DEV = 4
PAR_DEV = 2
NXY = 64
ROWS_DEV = 2048
ORDER = 131072
RHS = 2048
LEAVES = 256
PARENTS = 128
N_GX = 8
N_GY = 8


def draw_update_target(key, part):
    base = jax.random.fold_in(key, 11)
    key_one, key_two, key_three, key_four = jax.random.split(base, 4)
    groups = N_GX * N_GY
    perm_keys = jax.random.split(key_one, groups)
    orders = jax.vmap(lambda single: jax.random.permutation(single, N_GY))(perm_keys).astype(jnp.int32)
    positions = jnp.arange(LEAF_DEV, dtype=jnp.int32) % N_GY
    owners = orders[:, positions]
    within = jax.random.randint(key_two, (groups, LEAF_DEV), 0, PAR_DEV).astype(jnp.int32)
    parent = (owners * PAR_DEV + within).reshape(-1)
    total = LEAF_DEV * groups
    first = jax.random.randint(key_three, (total,), 0, 4).astype(jnp.int32)
    stride = jax.random.randint(key_four, (total,), 1, 4).astype(jnp.int32)
    second = (first + stride) % 4
    return jnp.stack([parent * 4 + first, parent * 4 + second], axis=1).astype(jnp.int32)


def block_scale(key, dims, pieces, smallest, largest):
    gain = 1.0
    for position, parts in pieces:
        steps = jax.random.uniform(jax.random.fold_in(jax.random.fold_in(key, 6), position), (parts,), jnp.float32, smallest / len(pieces), largest / len(pieces))
        gain = gain * jnp.repeat(jnp.exp(steps), dims[position] // parts).reshape((-1,) + (1,) * (len(dims) - 1 - position))
    return gain


def bell_draw(own_key, extent, width, limit, shards=(), held_as=jnp.bfloat16):
    values = jax.random.normal(own_key, extent, jnp.float32) * width
    if len(shards) > 0:
        values = block_scale(own_key, extent, shards, -0.22, 0.18) * values
    return jnp.clip(values, min=-limit, max=limit).astype(held_as)


def setup_inputs(seed: int = 0) -> dict:
    key_of = jax.random.split(jax.random.key(seed), 8)
    return {
        "right_side": bell_draw(key_of[0], (ORDER, RHS), 1.0, 6.0, ((0, 64), (1, 8)), jnp.float32),
        "send_order": jax.vmap(lambda own: jax.random.permutation(own, ROWS_DEV))(jax.random.split(key_of[1], NXY)).reshape((NXY, ROWS_DEV)).astype(jnp.int32),
        "recv_order": jax.vmap(lambda own: jax.random.permutation(own, ROWS_DEV))(jax.random.split(key_of[2], NXY)).reshape((NXY, ROWS_DEV)).astype(jnp.int32),
        "update_target": draw_update_target(jax.random.fold_in(key_of[7], 71), 0),
        "leaf_inv": bell_draw(key_of[4], (LEAVES, PIV, PIV), PIV ** -0.5, 0.375, ((0, 64), (1, 8)), jnp.float32),
        "leaf_low": bell_draw(key_of[5], (LEAVES, 2 * BLK, PIV), PIV ** -0.5, 0.375, ((0, 64), (1, 8)), jnp.float32),
        "parent_inv": bell_draw(key_of[6], (PARENTS, 4 * BLK, 4 * BLK), (4 * BLK) ** -0.5, 0.25, ((0, 64), (1, 8)), jnp.float32),
    }


def reference(right_side, send_order, recv_order, update_target, leaf_inv, leaf_low, parent_inv):
    nxy = N_GX * N_GY
    count = ROWS_DEV // nxy
    base = jnp.arange(nxy, dtype=jnp.int32)[:, None] * ROWS_DEV + send_order.astype(jnp.int32)
    routed = base.reshape(nxy, nxy, count).transpose(1, 0, 2).reshape(nxy, ROWS_DEV)
    picked = jnp.take_along_axis(routed, recv_order.astype(jnp.int32), axis=1).reshape(-1)
    front = right_side[picked].reshape(nxy, ROWS_DEV, RHS)
    leaf_rhs = front[:, :LEAF_DEV * PIV].reshape(LEAVES, PIV, RHS)
    parent_rhs = front[:, LEAF_DEV * PIV:].reshape(PARENTS, 4 * BLK, RHS)
    leaf_sol = jnp.einsum("fij,fjc->fic", leaf_inv, leaf_rhs, precision=lax.Precision.HIGHEST)
    update = jnp.einsum("fij,fjc->fic", leaf_low, leaf_sol, precision=lax.Precision.HIGHEST)
    group = jnp.arange(LEAVES, dtype=jnp.int32) // (LEAF_DEV * N_GY)
    targets = (group[:, None] * (PAR_DEV * N_GY * 4) + update_target.astype(jnp.int32)).reshape(-1)
    contribution = jax.ops.segment_sum(update.reshape(LEAVES * 2, BLK, RHS), targets, num_segments=PARENTS * 4)
    contribution = contribution.reshape(PARENTS, 4 * BLK, RHS)
    parent_sol = jnp.einsum("pij,pjc->pic", parent_inv, parent_rhs - contribution, precision=lax.Precision.HIGHEST)
    joined = jnp.concatenate([leaf_sol.reshape(nxy, LEAF_DEV * PIV, RHS), parent_sol.reshape(nxy, PAR_DEV * 4 * BLK, RHS)], axis=1)
    return joined.reshape(ORDER, RHS)
```

```python
import functools

import jax
import jax.numpy as jnp
from jax import lax
from jax.experimental import pallas as pl
from jax.experimental.pallas import tpu as pltpu
from jax.sharding import PartitionSpec as P

PIV = 256
BLK = 128
LEAF_DEV = 4
PAR_DEV = 2
OWN = PAR_DEV * 4
NX = 4
MESH = pl.DeviceIdType.MESH
Y_ORDER = (4, 1, 7, 2, 6, 3, 5, 0)
LANES = 128
HIGH = lax.Precision.HIGHEST


def dot(a, b):
    return jnp.dot(a, b, precision=HIGH, preferred_element_type=jnp.float32)


def kernel(
    n_gx, n_gy, n_gz,
    send_order, recv_order, target,
    rhs_hbm, inv_hbm, low_hbm, par_hbm,
    out,
    rhs_a, rhs_b, pack_a, pack_b, got_a, got_b, front_a, front_b,
    inv_all, low_all, par_all, upd, slots_a, slots_b, in_a, in_b,
    load_sem, z_send, z_recv, x_send, x_recv, f_send, f_recv,
    rows_send, rows_recv, upd_send, upd_recv,
):
    gx, gy, gz = lax.axis_index("gx"), lax.axis_index("gy"), lax.axis_index("gz")
    me = gx * n_gy + gy
    places = n_gx * n_gy
    share = rhs_a.shape[0] // places
    z_peer = gz + 1 - 2 * lax.rem(gz, 2)

    halves = (
        (rhs_a, pack_a, got_a, front_a, slots_a, in_a),
        (rhs_b, pack_b, got_b, front_b, slots_b, in_b),
    )
    loads = [
        pltpu.make_async_copy(rhs_hbm.at[:, pl.ds(0, LANES)], rhs_a, load_sem.at[0]),
        pltpu.make_async_copy(inv_hbm, inv_all.at[gz], load_sem.at[1]),
        pltpu.make_async_copy(low_hbm, low_all.at[gz], load_sem.at[2]),
        pltpu.make_async_copy(rhs_hbm.at[:, pl.ds(LANES, LANES)], rhs_b, load_sem.at[3]),
        pltpu.make_async_copy(par_hbm, par_all.at[gz], load_sem.at[4]),
    ]
    for load in loads:
        load.start()

    def place_of(i, j):
        other = lax.bitwise_xor(gx, lax.rem(i + j, n_gx))
        return other, lax.rem(gy + Y_ORDER[j], n_gy), lax.rem(i + j, n_gx)

    barrier = pltpu.get_barrier_semaphore()

    @pl.loop(0, n_gx)
    def _(i):
        for j in range(n_gy):
            px, py, turn = place_of(i, j)
            if Y_ORDER[j] == 0:
                @pl.when(turn != 0)
                def _():
                    pl.semaphore_signal(barrier, inc=1, device_id=(px, py, gz), device_id_type=MESH)
            else:
                pl.semaphore_signal(barrier, inc=1, device_id=(px, py, gz), device_id_type=MESH)

    def x_peer(k):
        return lax.rem(gz + 2 * k, n_gz)

    pl.semaphore_signal(barrier, inc=1, device_id=(gx, gy, z_peer), device_id_type=MESH)
    for k in range(1, NX):
        pl.semaphore_signal(barrier, inc=1, device_id=(gx, gy, x_peer(k)), device_id_type=MESH)

    def gather_rows(source, order, sink):
        @pl.loop(0, sink.shape[0] // share)
        def _(c):
            base = pl.multiple_of(c * share, share)
            for r in range(share):
                sink[pl.ds(base + r, 1), :] = source[pl.ds(order[base + r], 1), :]

    def send_rows(pack, got, h):
        got[pl.ds(pl.multiple_of(me * share, share), share), :] = pack[
            pl.ds(pl.multiple_of(me * share, share), share), :
        ]

        def send(px, py):
            there = px * n_gy + py
            pltpu.make_async_remote_copy(
                src_ref=pack.at[pl.ds(pl.multiple_of(there * share, share), share)],
                dst_ref=got.at[pl.ds(pl.multiple_of(me * share, share), share)],
                send_sem=rows_send.at[h],
                recv_sem=rows_recv.at[h],
                device_id=(px, py, gz),
                device_id_type=MESH,
            ).start()

        @pl.loop(0, n_gx)
        def _(i):
            for j in range(n_gy):
                px, py, turn = place_of(i, j)
                if Y_ORDER[j] == 0:
                    @pl.when(turn != 0)
                    def _():
                        send(px, py)
                else:
                    send(px, py)

    whole = (inv_all, low_all, par_all)

    def z_copy(w):
        return pltpu.make_async_remote_copy(
            src_ref=whole[w].at[gz], dst_ref=whole[w].at[gz],
            send_sem=z_send.at[w], recv_sem=z_recv.at[w],
            device_id=(gx, gy, z_peer), device_id_type=MESH,
        )

    def x_copy(w, k):
        return pltpu.make_async_remote_copy(
            src_ref=whole[w].at[gz], dst_ref=whole[w].at[gz],
            send_sem=x_send.at[w, k - 1], recv_sem=x_recv.at[w, k - 1],
            device_id=(gx, gy, x_peer(k)), device_id_type=MESH,
        )

    def f_copy(w, k):
        return pltpu.make_async_remote_copy(
            src_ref=whole[w].at[z_peer], dst_ref=whole[w].at[z_peer],
            send_sem=f_send.at[w, k - 1], recv_sem=f_recv.at[w, k - 1],
            device_id=(gx, gy, x_peer(k)), device_id_type=MESH,
        )

    def share_factor(w):
        z_copy(w).start()
        for k in (1, 3, 2):
            x_copy(w, k).start()

    def forward_factor(w):
        z_copy(w).wait_recv()
        for k in (1, 3, 2):
            f_copy(w, k).start()

    def await_factor(w):
        for k in range(1, NX):
            x_copy(w, k).wait_recv()
            f_copy(w, k).wait_recv()

    def splat(leaf, j):
        return jnp.full((8, LANES), target[leaf, j], jnp.int32)

    def owned_by(first, place):
        return jnp.logical_and(first >= place * OWN, first < place * OWN + OWN)

    def keep(mask, new, old):
        shape = new.shape
        tiles = (shape[0] // 8, 8, LANES)
        mask = jnp.broadcast_to(mask[None], tiles)
        return jnp.where(mask, new.reshape(tiles), old.reshape(tiles)).reshape(shape)

    def leaf_stage(h):
        got, front, slots, arriving = halves[h][2], halves[h][3], halves[h][4], halves[h][5]
        cols = pl.ds(h * LANES, LANES)
        gather_rows(got, recv_order, front)
        for l in range(LEAF_DEV):
            rows = pl.ds(l * PIV, PIV)
            sol = dot(inv_all[:, l].reshape(PIV, PIV), front[rows, :])
            out[rows, cols] = sol
            upd[h, l] = dot(low_all[:, l].reshape(PIV, PIV), sol)
        firsts = [splat(gy * LEAF_DEV + l, 0) for l in range(LEAF_DEV)]
        for step in Y_ORDER:
            there = lax.rem(gy + step, n_gy)
            masks = [owned_by(firsts[l], there) for l in range(1, LEAF_DEV)]
            for part in range(0, PIV, BLK):
                rows = pl.ds(part, BLK)
                chosen = upd[h, 0, rows, :]
                for l in range(1, LEAF_DEV):
                    chosen = keep(masks[l - 1], upd[h, l, rows, :], chosen)
                if step == 0:
                    arriving[gy, rows, :] = chosen
                else:
                    slots[step, rows, :] = chosen
        for step in Y_ORDER:
            if step:
                there = lax.rem(gy + step, n_gy)
                pltpu.make_async_remote_copy(
                    src_ref=slots.at[step], dst_ref=arriving.at[gy],
                    send_sem=upd_send.at[h], recv_sem=upd_recv.at[h],
                    device_id=(gx, there, gz), device_id_type=MESH,
                ).start()

    def parent_stage(h):
        front, arriving = halves[h][3], halves[h][5]
        cols = pl.ds(h * LANES, LANES)
        zeros = jnp.zeros((BLK, LANES), jnp.float32)
        first, second = [], []
        for s in range(n_gy):
            one = two = jnp.full((8, LANES), -1, jnp.int32)
            for l in range(LEAF_DEV):
                t_one, t_two = splat(s * LEAF_DEV + l, 0), splat(s * LEAF_DEV + l, 1)
                mine = owned_by(t_one, gy)
                one = jnp.where(mine, t_one, one)
                two = jnp.where(mine, t_two, two)
            first.append(one)
            second.append(two)
        for p in range(PAR_DEV):
            for q in range(4):
                b = p * 4 + q
                here = gy * OWN + b
                total = zeros
                for s in range(n_gy):
                    piece = keep(second[s] == here, arriving[s, pl.ds(BLK, BLK), :], zeros)
                    total = total + keep(first[s] == here, arriving[s, pl.ds(0, BLK), :], piece)
                rows = pl.ds(LEAF_DEV * PIV + b * BLK, BLK)
                front[rows, :] = front[rows, :] - total
        for p in range(PAR_DEV):
            rows = pl.ds(LEAF_DEV * PIV + p * 4 * BLK, 4 * BLK)
            out[rows, cols] = dot(par_all[:, p].reshape(4 * BLK, 4 * BLK), front[rows, :])

    def bulk(ref, sem, count):
        part = ref.at[pl.ds(0, count)]
        return pltpu.make_async_copy(part, part, sem)

    others = (places - 1) * share
    loads[0].wait()
    gather_rows(rhs_a, send_order, pack_a)
    loads[1].wait()
    loads[2].wait()
    pl.semaphore_wait(barrier, places - 1 + NX)
    share_factor(0)
    share_factor(1)
    send_rows(pack_a, got_a, 0)
    loads[3].wait()
    gather_rows(rhs_b, send_order, pack_b)
    send_rows(pack_b, got_b, 1)
    loads[4].wait()
    share_factor(2)
    forward_factor(0)
    forward_factor(1)
    bulk(got_a, rows_recv.at[0], others).wait()
    await_factor(0)
    await_factor(1)
    leaf_stage(0)
    forward_factor(2)
    bulk(got_b, rows_recv.at[1], others).wait()
    leaf_stage(1)
    await_factor(2)
    bulk(in_a, upd_recv.at[0], n_gy - 1).wait()
    parent_stage(0)
    bulk(in_b, upd_recv.at[1], n_gy - 1).wait()
    parent_stage(1)
    for w in range(3):
        z_copy(w).wait_send()
        for k in range(1, NX):
            x_copy(w, k).wait_send()
            f_copy(w, k).wait_send()
    for h in range(2):
        bulk(halves[h][1], rows_send.at[h], others).wait()
        bulk(halves[h][4], upd_send.at[h], n_gy - 1).wait()


def body(sizes, right_side, send_order, recv_order, update_target, leaf_inv, leaf_low, parent_inv):
    n_gx, n_gy, n_gz = sizes
    rows = right_side.shape[0]
    f32 = jnp.float32
    any_space = pl.BlockSpec(memory_space=pl.ANY)
    smem = pl.BlockSpec(memory_space=pltpu.SMEM)
    half = pltpu.VMEM((rows, LANES), f32)
    dma = pltpu.SemaphoreType.DMA
    return pl.pallas_call(
        functools.partial(kernel, n_gx, n_gy, n_gz),
        out_shape=jax.ShapeDtypeStruct(right_side.shape, f32),
        in_specs=[smem, smem, smem, any_space, any_space, any_space, any_space],
        out_specs=pl.BlockSpec(memory_space=pltpu.VMEM),
        scratch_shapes=[
            half, half, half, half, half, half, half, half,
            pltpu.VMEM((n_gz,) + leaf_inv.shape, f32),
            pltpu.VMEM((n_gz,) + leaf_low.shape, f32),
            pltpu.VMEM((n_gz,) + parent_inv.shape, f32),
            pltpu.VMEM((2, LEAF_DEV, PIV, LANES), f32),
            pltpu.VMEM((n_gy, PIV, LANES), f32),
            pltpu.VMEM((n_gy, PIV, LANES), f32),
            pltpu.VMEM((n_gy, PIV, LANES), f32),
            pltpu.VMEM((n_gy, PIV, LANES), f32),
            dma((5,)), dma((3,)), dma((3,)),
            dma((3, NX - 1)), dma((3, NX - 1)), dma((3, NX - 1)), dma((3, NX - 1)),
            dma((2,)), dma((2,)), dma((2,)), dma((2,)),
        ],
        compiler_params=pltpu.CompilerParams(
            collective_id=0, has_side_effects=True, vmem_limit_bytes=56 * 2**20
        ),
        name="forward_solve",
    )(
        send_order.reshape(-1), recv_order.reshape(-1), update_target,
        right_side, leaf_inv, leaf_low, parent_inv,
    )


def solution(mesh):
    sizes = (mesh.shape["gx"], mesh.shape["gy"], mesh.shape["gz"])
    placed = (
        P(("gx", "gy"), "gz"),
        P(("gx", "gy"), None),
        P(("gx", "gy"), None),
        P("gx", None),
        P(("gx", "gy"), "gz", None),
        P(("gx", "gy"), "gz", None),
        P(("gx", "gy"), "gz", None),
    )
    return jax.shard_map(
        functools.partial(body, sizes), mesh=mesh, in_specs=placed,
        out_specs=P(("gx", "gy"), "gz"), check_vma=False,
    )
```

```python
import functools

import jax
import jax.numpy as jnp
from jax import lax
from jax.experimental import pallas as pl
from jax.experimental.pallas import tpu as pltpu
from jax.sharding import PartitionSpec as P

PIV = 256
BLK = 128
LEAF_DEV = 4
PAR_DEV = 2
OWN = PAR_DEV * 4
NX = 4
MESH = pl.DeviceIdType.MESH
Y_ORDER = (4, 3, 5, 2, 6, 1, 7)
G_FAR = (6, 7, 4, 5)
G_NEAR = (2, 3, 1)
LANES = 128
HIGH = lax.Precision.HIGHEST


def dot(a, b):
    return jnp.dot(a, b, precision=HIGH, preferred_element_type=jnp.float32)


def kernel(
    n_gx, n_gy, n_gz,
    send_order, recv_order, target,
    rhs_hbm, inv_hbm, low_hbm, par_hbm,
    out,
    rhs_a, rhs_b, pack_a, pack_b, mid_a, mid_b, got_a, got_b, front_a, front_b,
    inv_all, low_all, par_all, upd, slots_a, slots_b, in_a, in_b,
    load_sem, z_send, z_recv, x_send, x_recv, f_send, f_recv,
    y_send, y_recv, g_send, g_recv, upd_send, upd_recv,
):
    gx, gy, gz = lax.axis_index("gx"), lax.axis_index("gy"), lax.axis_index("gz")
    part = n_gx // 2
    share = rhs_a.shape[0] // (n_gx * n_gy)
    lot = n_gy * share
    z_peer = gz + 1 - 2 * lax.rem(gz, 2)
    near = gx // part
    far = 1 - near

    rhs, pack, mid = (rhs_a, rhs_b), (pack_a, pack_b), (mid_a, mid_b)
    got, front = (got_a, got_b), (front_a, front_b)
    slots, arrived = (slots_a, slots_b), (in_a, in_b)
    loads = [
        pltpu.make_async_copy(rhs_hbm.at[:, pl.ds(0, LANES)], rhs_a, load_sem.at[0]),
        pltpu.make_async_copy(inv_hbm, inv_all.at[gz], load_sem.at[1]),
        pltpu.make_async_copy(low_hbm, low_all.at[gz], load_sem.at[2]),
        pltpu.make_async_copy(rhs_hbm.at[:, pl.ds(LANES, LANES)], rhs_b, load_sem.at[3]),
        pltpu.make_async_copy(par_hbm, par_all.at[gz], load_sem.at[4]),
    ]
    for load in loads:
        load.start()

    barrier = pltpu.get_barrier_semaphore()

    def greet(px, py, pz):
        pl.semaphore_signal(barrier, inc=1, device_id=(px, py, pz), device_id_type=MESH)

    def x_peer(k):
        return lax.rem(gz + 2 * k, n_gz)

    for step in Y_ORDER:
        greet(gx, lax.rem(gy + step, n_gy), gz)
    for turn in G_FAR + G_NEAR:
        greet(lax.bitwise_xor(gx, turn), gy, gz)
    greet(gx, gy, z_peer)
    for k in range(1, NX):
        greet(gx, gy, x_peer(k))

    def pick_rows(h, side):
        @pl.loop(0, part)
        def _(i):
            for y in range(n_gy):
                place = (side * part + i) * n_gy + y
                base = place * share

                @pl.loop(0, share // 8)
                def _(t):
                    for r in range(8):
                        at = t * 8 + r
                        pack[h][side * part + i, pl.ds(y * share + at, 1), :] = rhs[h][
                            pl.ds(send_order[base + at], 1), :
                        ]

    def send_along_y(h, side, far_or_near):
        places = pl.ds(pl.multiple_of(side * part, part), part)
        own = pl.ds(pl.multiple_of(gy * share, share), share)
        for step in Y_ORDER:
            there = lax.rem(gy + step, n_gy)
            pltpu.make_async_remote_copy(
                src_ref=pack[h].at[places, pl.ds(pl.multiple_of(there * share, share), share)],
                dst_ref=mid[h].at[places, own],
                send_sem=y_send.at[h],
                recv_sem=y_recv.at[h, far_or_near],
                device_id=(gx, there, gz),
                device_id_type=MESH,
            ).start()
        mid[h][places, own, :] = pack[h][places, own, :]

    def await_y(h, far_or_near):
        bulk(mid[h].at[pl.ds(0, part), pl.ds(0, (n_gy - 1) * share)], y_recv.at[h, far_or_near])

    def send_along_gx(h, turns, far_or_near):
        own = pl.ds(pl.multiple_of(gx * lot, lot), lot)
        for turn in turns:
            there = lax.bitwise_xor(gx, turn)
            pltpu.make_async_remote_copy(
                src_ref=mid[h].at[there],
                dst_ref=got[h].at[own],
                send_sem=g_send.at[h],
                recv_sem=g_recv.at[h, far_or_near],
                device_id=(there, gy, gz),
                device_id_type=MESH,
            ).start()

    def keep_own(h):
        got[h][pl.ds(pl.multiple_of(gx * lot, lot), lot), :] = mid[h][gx]

    def await_gx(h):
        bulk(got[h].at[pl.ds(0, len(G_FAR) * lot)], g_recv.at[h, 0])
        bulk(got[h].at[pl.ds(0, len(G_NEAR) * lot)], g_recv.at[h, 1])

    def bulk(view, sem):
        pltpu.make_async_copy(view, view, sem).wait()

    def take_rows(h):
        @pl.loop(0, front[h].shape[0] // 32)
        def _(c):
            base = pl.multiple_of(c * 32, 32)
            for r in range(32):
                front[h][pl.ds(base + r, 1), :] = got[h][pl.ds(recv_order[base + r], 1), :]

    whole = (inv_all, low_all, par_all)

    def z_copy(w):
        return pltpu.make_async_remote_copy(
            src_ref=whole[w].at[gz], dst_ref=whole[w].at[gz],
            send_sem=z_send.at[w], recv_sem=z_recv.at[w],
            device_id=(gx, gy, z_peer), device_id_type=MESH,
        )

    def x_copy(w, k):
        return pltpu.make_async_remote_copy(
            src_ref=whole[w].at[gz], dst_ref=whole[w].at[gz],
            send_sem=x_send.at[w, k - 1], recv_sem=x_recv.at[w, k - 1],
            device_id=(gx, gy, x_peer(k)), device_id_type=MESH,
        )

    def f_copy(w, k):
        return pltpu.make_async_remote_copy(
            src_ref=whole[w].at[z_peer], dst_ref=whole[w].at[z_peer],
            send_sem=f_send.at[w, k - 1], recv_sem=f_recv.at[w, k - 1],
            device_id=(gx, gy, x_peer(k)), device_id_type=MESH,
        )

    def share_along_x(w):
        for k in (1, 3, 2):
            x_copy(w, k).start()

    def forward_factor(w):
        z_copy(w).wait_recv()
        for k in (1, 3, 2):
            f_copy(w, k).start()

    def await_factor(w):
        for k in range(1, NX):
            x_copy(w, k).wait_recv()
            f_copy(w, k).wait_recv()

    def splat(leaf, j):
        return jnp.full((8, LANES), target[j, leaf], jnp.int32)

    def owned_by(first, place):
        return jnp.logical_and(first >= place * OWN, first < place * OWN + OWN)

    def keep(mask, new, old):
        shape = new.shape
        tiles = (shape[0] // 8, 8, LANES)
        mask = jnp.broadcast_to(mask[None], tiles)
        return jnp.where(mask, new.reshape(tiles), old.reshape(tiles)).reshape(shape)

    def leaf_stage(h):
        cols = pl.ds(h * LANES, LANES)
        take_rows(h)
        for l in range(LEAF_DEV):
            rows = pl.ds(l * PIV, PIV)
            sol = dot(inv_all[:, l].reshape(PIV, PIV), front[h][rows, :])
            out[rows, cols] = sol
            upd[h, l] = dot(low_all[:, l].reshape(PIV, PIV), sol)
        firsts = [splat(gy * LEAF_DEV + l, 0) for l in range(LEAF_DEV)]
        for step in Y_ORDER + (0,):
            there = lax.rem(gy + step, n_gy)
            masks = [owned_by(firsts[l], there) for l in range(1, LEAF_DEV)]
            for part in range(0, PIV, BLK):
                rows = pl.ds(part, BLK)
                chosen = upd[h, 0, rows, :]
                for l in range(1, LEAF_DEV):
                    chosen = keep(masks[l - 1], upd[h, l, rows, :], chosen)
                if step == 0:
                    arrived[h][gy, rows, :] = chosen
                else:
                    slots[h][step, rows, :] = chosen
        for step in Y_ORDER:
            pltpu.make_async_remote_copy(
                src_ref=slots[h].at[step], dst_ref=arrived[h].at[gy],
                send_sem=upd_send.at[h], recv_sem=upd_recv.at[h],
                device_id=(gx, lax.rem(gy + step, n_gy), gz), device_id_type=MESH,
            ).start()

    def parent_stage(h):
        cols = pl.ds(h * LANES, LANES)
        zeros = jnp.zeros((BLK, LANES), jnp.float32)
        first, second = [], []
        for s in range(n_gy):
            one = two = jnp.full((8, LANES), -1, jnp.int32)
            for l in range(LEAF_DEV):
                t_one, t_two = splat(s * LEAF_DEV + l, 0), splat(s * LEAF_DEV + l, 1)
                mine = owned_by(t_one, gy)
                one = jnp.where(mine, t_one, one)
                two = jnp.where(mine, t_two, two)
            first.append(one)
            second.append(two)
        for p in range(PAR_DEV):
            for q in range(4):
                b = p * 4 + q
                here = gy * OWN + b
                total = zeros
                for s in range(n_gy):
                    piece = keep(second[s] == here, arrived[h][s, pl.ds(BLK, BLK), :], zeros)
                    total = total + keep(first[s] == here, arrived[h][s, pl.ds(0, BLK), :], piece)
                rows = pl.ds(LEAF_DEV * PIV + b * BLK, BLK)
                front[h][rows, :] = front[h][rows, :] - total
        for p in range(PAR_DEV):
            rows = pl.ds(LEAF_DEV * PIV + p * 4 * BLK, 4 * BLK)
            out[rows, cols] = dot(par_all[:, p].reshape(4 * BLK, 4 * BLK), front[h][rows, :])

    loads[0].wait()
    pick_rows(0, far)
    loads[1].wait()
    loads[2].wait()
    pl.semaphore_wait(barrier, n_gx + n_gy - 2 + NX)
    z_copy(0).start()
    z_copy(1).start()
    send_along_y(0, far, 0)
    share_along_x(0)
    share_along_x(1)
    pick_rows(0, near)
    send_along_y(0, near, 1)
    loads[3].wait()
    pick_rows(1, far)
    pick_rows(1, near)
    loads[4].wait()
    share_along_x(2)
    await_y(0, 0)
    send_along_gx(0, G_FAR, 0)
    send_along_y(1, far, 0)
    forward_factor(0)
    forward_factor(1)
    await_y(0, 1)
    send_along_gx(0, G_NEAR, 1)
    send_along_y(1, near, 1)
    keep_own(0)
    await_gx(0)
    await_y(1, 0)
    send_along_gx(1, G_FAR, 0)
    await_factor(0)
    await_factor(1)
    leaf_stage(0)
    await_y(1, 1)
    send_along_gx(1, G_NEAR, 1)
    keep_own(1)
    await_gx(1)
    z_copy(2).start()
    leaf_stage(1)
    forward_factor(2)
    await_factor(2)
    bulk(in_a.at[pl.ds(0, n_gy - 1)], upd_recv.at[0])
    parent_stage(0)
    bulk(in_b.at[pl.ds(0, n_gy - 1)], upd_recv.at[1])
    parent_stage(1)
    for w in range(3):
        z_copy(w).wait_send()
        for k in range(1, NX):
            x_copy(w, k).wait_send()
            f_copy(w, k).wait_send()
    for h in range(2):
        bulk(mid[h].at[:, pl.ds(0, (n_gy - 1) * share)], y_send.at[h])
        bulk(got[h].at[pl.ds(0, (n_gx - 1) * lot)], g_send.at[h])
        bulk(slots[h].at[pl.ds(0, n_gy - 1)], upd_send.at[h])


def body(sizes, right_side, send_order, recv_order, update_target, leaf_inv, leaf_low, parent_inv):
    n_gx, n_gy, n_gz = sizes
    rows = right_side.shape[0]
    f32 = jnp.float32
    any_space = pl.BlockSpec(memory_space=pl.ANY)
    smem = pl.BlockSpec(memory_space=pltpu.SMEM)
    half = pltpu.VMEM((rows, LANES), f32)
    lots = pltpu.VMEM((n_gx, rows // n_gx, LANES), f32)
    dma = pltpu.SemaphoreType.DMA
    return pl.pallas_call(
        functools.partial(kernel, n_gx, n_gy, n_gz),
        out_shape=pltpu.VMEM(right_side.shape, f32),
        in_specs=[smem, smem, smem, any_space, any_space, any_space, any_space],
        out_specs=pl.BlockSpec(memory_space=pltpu.VMEM),
        scratch_shapes=[
            half, half, lots, lots, lots, lots, half, half, half, half,
            pltpu.VMEM((n_gz,) + leaf_inv.shape, f32),
            pltpu.VMEM((n_gz,) + leaf_low.shape, f32),
            pltpu.VMEM((n_gz,) + parent_inv.shape, f32),
            pltpu.VMEM((2, LEAF_DEV, PIV, LANES), f32),
            pltpu.VMEM((n_gy, PIV, LANES), f32),
            pltpu.VMEM((n_gy, PIV, LANES), f32),
            pltpu.VMEM((n_gy, PIV, LANES), f32),
            pltpu.VMEM((n_gy, PIV, LANES), f32),
            dma((5,)), dma((3,)), dma((3,)),
            dma((3, NX - 1)), dma((3, NX - 1)), dma((3, NX - 1)), dma((3, NX - 1)),
            dma((2,)), dma((2, 2)), dma((2,)), dma((2, 2)), dma((2,)), dma((2,)),
        ],
        compiler_params=pltpu.CompilerParams(
            collective_id=0, has_side_effects=True, vmem_limit_bytes=61 * 2**20 + 7 * 2**17
        ),
        name="forward_solve",
    )(
        send_order.reshape(-1), recv_order.reshape(-1), update_target.T,
        right_side, leaf_inv, leaf_low, parent_inv,
    )


def solution(mesh):
    sizes = (mesh.shape["gx"], mesh.shape["gy"], mesh.shape["gz"])
    placed = (
        P(("gx", "gy"), "gz"),
        P(("gx", "gy"), None),
        P(("gx", "gy"), None),
        P("gx", None),
        P(("gx", "gy"), "gz", None),
        P(("gx", "gy"), "gz", None),
        P(("gx", "gy"), "gz", None),
    )
    return jax.shard_map(
        functools.partial(body, sizes), mesh=mesh, in_specs=placed,
        out_specs=P(("gx", "gy"), "gz"), check_vma=False,
    )
```

```python
import functools

import jax
import jax.numpy as jnp
from jax import lax
from jax.experimental import pallas as pl
from jax.experimental.pallas import tpu as pltpu
from jax.sharding import PartitionSpec as P

PIV = 256
BLK = 128
LEAF_DEV = 4
PAR_DEV = 2
OWN = PAR_DEV * 4
NX = 4
MESH = pl.DeviceIdType.MESH
Y_ORDER = (4, 3, 5, 2, 6, 1, 7)
G_FAR = (6, 7, 4, 5)
G_NEAR = (2, 3, 1)
LANES = 128
HIGH = lax.Precision.HIGHEST


def dot(a, b):
    return jnp.dot(a, b, precision=HIGH, preferred_element_type=jnp.float32)


def kernel(
    n_gx, n_gy, n_gz,
    send_hbm, recv_hbm, target_hbm,
    rhs_hbm, inv_hbm, low_hbm, par_hbm,
    out,
    rhs_a, rhs_b, pack_a, pack_b, mid_a, mid_b, got_a, got_b, front_a, front_b,
    inv_all, low_all, par_all, upd, slots_a, slots_b, in_a, in_b,
    par_hi, par_lo, send_order, recv_order, target,
    load_sem, z_send, z_recv, x_send, x_recv, f_send, f_recv,
    y_send, y_recv, g_send, g_recv, upd_send, upd_recv,
):
    gx, gy, gz = lax.axis_index("gx"), lax.axis_index("gy"), lax.axis_index("gz")
    part = n_gx // 2
    share = rhs_a.shape[0] // (n_gx * n_gy)
    lot = n_gy * share
    z_peer = gz + 1 - 2 * lax.rem(gz, 2)
    near = gx // part
    far = 1 - near

    rhs, pack, mid = (rhs_a, rhs_b), (pack_a, pack_b), (mid_a, mid_b)
    got, front = (got_a, got_b), (front_a, front_b)
    slots, arrived = (slots_a, slots_b), (in_a, in_b)
    loads = [
        pltpu.make_async_copy(rhs_hbm.at[:, pl.ds(0, LANES)], rhs_a, load_sem.at[0]),
        pltpu.make_async_copy(inv_hbm, inv_all.at[gz], load_sem.at[1]),
        pltpu.make_async_copy(low_hbm, low_all.at[gz], load_sem.at[2]),
        pltpu.make_async_copy(rhs_hbm.at[:, pl.ds(LANES, LANES)], rhs_b, load_sem.at[3]),
        pltpu.make_async_copy(par_hbm, par_all.at[gz], load_sem.at[4]),
        pltpu.make_async_copy(send_hbm, send_order, load_sem.at[5]),
        pltpu.make_async_copy(recv_hbm, recv_order, load_sem.at[6]),
        pltpu.make_async_copy(target_hbm, target, load_sem.at[7]),
    ]
    for n in (5, 0, 1, 2, 4, 3, 6, 7):
        loads[n].start()

    barrier = pltpu.get_barrier_semaphore()

    def greet(px, py, pz):
        pl.semaphore_signal(barrier, inc=1, device_id=(px, py, pz), device_id_type=MESH)

    def x_peer(k):
        return lax.rem(gz + 2 * k, n_gz)

    for step in Y_ORDER:
        greet(gx, lax.rem(gy + step, n_gy), gz)
    for turn in G_FAR + G_NEAR:
        greet(lax.bitwise_xor(gx, turn), gy, gz)
    greet(gx, gy, z_peer)
    for k in range(1, NX):
        greet(gx, gy, x_peer(k))

    def turn_of(j):
        away = (j + 1) // 2
        return n_gy // 2 + away * (1 - 2 * lax.rem(j, 2))

    def pick_and_send_along_y(h, side, far_or_near):
        places = pl.ds(pl.multiple_of(side * part, part), part)
        own = pl.ds(pl.multiple_of(gy * share, share), share)

        @pl.loop(0, n_gy)
        def _(j):
            there = lax.rem(gy + turn_of(j), n_gy)

            @pl.loop(0, part)
            def _(i):
                place = side * part + i
                base = (place * n_gy + there) * share
                at = pl.multiple_of(there * share, share)
                for r in range(share):
                    pack[h][place, pl.ds(at + r, 1), :] = rhs[h][pl.ds(send_order[base + r], 1), :]

            @pl.when(j > 0)
            def _():
                ready = lax.rem(gy + turn_of(j - 1), n_gy)
                pltpu.make_async_remote_copy(
                    src_ref=pack[h].at[places, pl.ds(pl.multiple_of(ready * share, share), share)],
                    dst_ref=mid[h].at[places, own],
                    send_sem=y_send.at[h],
                    recv_sem=y_recv.at[h, far_or_near],
                    device_id=(gx, ready, gz),
                    device_id_type=MESH,
                ).start()

        mid[h][places, own, :] = pack[h][places, own, :]

    def pick_rows(h, side):
        @pl.loop(0, part * n_gy)
        def _(c):
            place = side * part + c // n_gy
            at = pl.multiple_of(lax.rem(c, n_gy) * share, share)
            base = place * lot + at
            for r in range(share):
                pack[h][place, pl.ds(at + r, 1), :] = rhs[h][pl.ds(send_order[base + r], 1), :]

    def send_along_y(h, side, far_or_near):
        places = pl.ds(pl.multiple_of(side * part, part), part)
        own = pl.ds(pl.multiple_of(gy * share, share), share)
        for step in Y_ORDER:
            there = lax.rem(gy + step, n_gy)
            pltpu.make_async_remote_copy(
                src_ref=pack[h].at[places, pl.ds(pl.multiple_of(there * share, share), share)],
                dst_ref=mid[h].at[places, own],
                send_sem=y_send.at[h],
                recv_sem=y_recv.at[h, far_or_near],
                device_id=(gx, there, gz),
                device_id_type=MESH,
            ).start()
        mid[h][places, own, :] = pack[h][places, own, :]

    def await_y(h, far_or_near):
        bulk(mid[h].at[pl.ds(0, part), pl.ds(0, (n_gy - 1) * share)], y_recv.at[h, far_or_near])

    def send_along_gx(h, turns, far_or_near):
        own = pl.ds(pl.multiple_of(gx * lot, lot), lot)
        for turn in turns:
            there = lax.bitwise_xor(gx, turn)
            pltpu.make_async_remote_copy(
                src_ref=mid[h].at[there],
                dst_ref=got[h].at[own],
                send_sem=g_send.at[h],
                recv_sem=g_recv.at[h, far_or_near],
                device_id=(there, gy, gz),
                device_id_type=MESH,
            ).start()

    def keep_own(h):
        got[h][pl.ds(pl.multiple_of(gx * lot, lot), lot), :] = mid[h][gx]

    def await_gx(h):
        bulk(got[h].at[pl.ds(0, len(G_FAR) * lot)], g_recv.at[h, 0])
        bulk(got[h].at[pl.ds(0, len(G_NEAR) * lot)], g_recv.at[h, 1])

    def bulk(view, sem):
        pltpu.make_async_copy(view, view, sem).wait()

    def take_rows(h):
        @pl.loop(0, front[h].shape[0] // 32)
        def _(c):
            base = pl.multiple_of(c * 32, 32)
            for r in range(32):
                front[h][pl.ds(base + r, 1), :] = got[h][pl.ds(recv_order[base + r], 1), :]

    whole = (inv_all, low_all, par_all)

    def z_copy(w):
        return pltpu.make_async_remote_copy(
            src_ref=whole[w].at[gz], dst_ref=whole[w].at[gz],
            send_sem=z_send.at[w], recv_sem=z_recv.at[w],
            device_id=(gx, gy, z_peer), device_id_type=MESH,
        )

    def x_copy(w, k):
        return pltpu.make_async_remote_copy(
            src_ref=whole[w].at[gz], dst_ref=whole[w].at[gz],
            send_sem=x_send.at[w, k - 1], recv_sem=x_recv.at[w, k - 1],
            device_id=(gx, gy, x_peer(k)), device_id_type=MESH,
        )

    def f_copy(w, k):
        return pltpu.make_async_remote_copy(
            src_ref=whole[w].at[z_peer], dst_ref=whole[w].at[z_peer],
            send_sem=f_send.at[w, k - 1], recv_sem=f_recv.at[w, k - 1],
            device_id=(gx, gy, x_peer(k)), device_id_type=MESH,
        )

    def share_along_x(w):
        for k in (1, 3, 2):
            x_copy(w, k).start()

    def forward_factor(w):
        z_copy(w).wait_recv()
        for k in (1, 3, 2):
            f_copy(w, k).start()

    def await_factor(w):
        for k in range(1, NX):
            x_copy(w, k).wait_recv()
            f_copy(w, k).wait_recv()

    def splat(leaf, j):
        return jnp.full((8, LANES), target[j, leaf], jnp.int32)

    def owned_by(first, place):
        return jnp.logical_and(first >= place * OWN, first < place * OWN + OWN)

    def keep(mask, new, old):
        shape = new.shape
        tiles = (shape[0] // 8, 8, LANES)
        mask = jnp.broadcast_to(mask[None], tiles)
        return jnp.where(mask, new.reshape(tiles), old.reshape(tiles)).reshape(shape)

    def leaf_stage(h):
        cols = pl.ds(h * LANES, LANES)
        take_rows(h)
        for l in range(LEAF_DEV):
            rows = pl.ds(l * PIV, PIV)
            sol = dot(inv_all[:, l].reshape(PIV, PIV), front[h][rows, :])
            out[rows, cols] = sol
            upd[h, l] = dot(low_all[:, l].reshape(PIV, PIV), sol)
        firsts = [splat(gy * LEAF_DEV + l, 0) for l in range(LEAF_DEV)]
        for step in Y_ORDER + (0,):
            there = lax.rem(gy + step, n_gy)
            masks = [owned_by(firsts[l], there) for l in range(1, LEAF_DEV)]
            for part in range(0, PIV, BLK):
                rows = pl.ds(part, BLK)
                chosen = upd[h, 0, rows, :]
                for l in range(1, LEAF_DEV):
                    chosen = keep(masks[l - 1], upd[h, l, rows, :], chosen)
                if step == 0:
                    arrived[h][gy, rows, :] = chosen
                else:
                    slots[h][step, rows, :] = chosen
        for step in Y_ORDER:
            pltpu.make_async_remote_copy(
                src_ref=slots[h].at[step], dst_ref=arrived[h].at[gy],
                send_sem=upd_send.at[h], recv_sem=upd_recv.at[h, step],
                device_id=(gx, lax.rem(gy + step, n_gy), gz), device_id_type=MESH,
            ).start()

    def absorb(h, source):
        zeros = jnp.zeros((BLK, LANES), jnp.float32)
        one = two = jnp.full((8, LANES), -1, jnp.int32)
        for l in range(LEAF_DEV):
            leaf = source * LEAF_DEV + l
            t_one, t_two = splat(leaf, 0), splat(leaf, 1)
            mine = owned_by(t_one, gy)
            one = jnp.where(mine, t_one, one)
            two = jnp.where(mine, t_two, two)
        for b in range(OWN):
            here = gy * OWN + b
            rows = pl.ds(LEAF_DEV * PIV + b * BLK, BLK)
            piece = keep(two == here, arrived[h][source, pl.ds(BLK, BLK), :], zeros)
            piece = keep(one == here, arrived[h][source, pl.ds(0, BLK), :], piece)
            front[h][rows, :] = front[h][rows, :] - piece

    def absorb_all(h):
        absorb(h, gy)

        @pl.loop(0, n_gy - 1)
        def _(j):
            turn = turn_of(j)
            source = lax.rem(gy + n_gy - turn, n_gy)
            pltpu.make_async_copy(
                arrived[h].at[source], arrived[h].at[source], upd_recv.at[h, turn]
            ).wait()
            absorb(h, source)

    def split(x):
        high = x.astype(jnp.bfloat16)
        return high, (x - high.astype(jnp.float32)).astype(jnp.bfloat16)

    def split_parents():
        for p in range(PAR_DEV):
            rows = par_all.shape[2]
            for g in range(n_gz):
                at = pl.ds(g * rows, rows)
                par_hi[p, at, :], par_lo[p, at, :] = split(par_all[g, p])

    def parent_stage(h):
        absorb_all(h)
        cols = pl.ds(h * LANES, LANES)
        for p in range(PAR_DEV):
            rows = pl.ds(LEAF_DEV * PIV + p * 4 * BLK, 4 * BLK)
            high, low = split(front[h][rows, :])
            both = jnp.dot(
                par_hi[p], jnp.concatenate([high, low], axis=1), preferred_element_type=jnp.float32
            )
            rest = jnp.dot(par_lo[p], high, preferred_element_type=jnp.float32)
            out[rows, cols] = both[:, :LANES] + both[:, LANES:] + rest

    loads[1].wait()
    loads[2].wait()
    loads[4].wait()
    loads[5].wait()
    loads[0].wait()
    pl.semaphore_wait(barrier, n_gx + n_gy - 2 + NX)
    z_copy(0).start()
    z_copy(1).start()
    pick_and_send_along_y(0, far, 0)
    for w in range(3):
        share_along_x(w)
    pick_and_send_along_y(0, near, 1)
    loads[3].wait()
    pick_rows(1, far)
    pick_rows(1, near)
    loads[6].wait()
    loads[7].wait()
    await_y(0, 0)
    send_along_gx(0, G_FAR, 0)
    send_along_y(1, far, 0)
    forward_factor(0)
    forward_factor(1)
    await_y(0, 1)
    send_along_gx(0, G_NEAR, 1)
    send_along_y(1, near, 1)
    keep_own(0)
    await_gx(0)
    await_y(1, 0)
    send_along_gx(1, G_FAR, 0)
    await_factor(0)
    await_factor(1)
    leaf_stage(0)
    await_y(1, 1)
    send_along_gx(1, G_NEAR, 1)
    keep_own(1)
    await_gx(1)
    z_copy(2).start()
    leaf_stage(1)
    forward_factor(2)
    await_factor(2)
    split_parents()
    parent_stage(0)
    parent_stage(1)
    for w in range(3):
        z_copy(w).wait_send()
        for k in range(1, NX):
            x_copy(w, k).wait_send()
            f_copy(w, k).wait_send()
    for h in range(2):
        bulk(mid[h].at[:, pl.ds(0, (n_gy - 1) * share)], y_send.at[h])
        bulk(got[h].at[pl.ds(0, (n_gx - 1) * lot)], g_send.at[h])
        bulk(slots[h].at[pl.ds(0, n_gy - 1)], upd_send.at[h])


def body(sizes, right_side, send_order, recv_order, update_target, leaf_inv, leaf_low, parent_inv):
    n_gx, n_gy, n_gz = sizes
    rows = right_side.shape[0]
    f32 = jnp.float32
    any_space = pl.BlockSpec(memory_space=pl.ANY)
    half = pltpu.VMEM((rows, LANES), f32)
    lots = pltpu.VMEM((n_gx, rows // n_gx, LANES), f32)
    dma = pltpu.SemaphoreType.DMA
    return pl.pallas_call(
        functools.partial(kernel, n_gx, n_gy, n_gz),
        out_shape=pltpu.VMEM(right_side.shape, f32),
        in_specs=[any_space, any_space, any_space, any_space, any_space, any_space, any_space],
        out_specs=pl.BlockSpec(memory_space=pltpu.VMEM),
        scratch_shapes=[
            half, half, lots, lots, lots, lots, half, half, half, half,
            pltpu.VMEM((n_gz,) + leaf_inv.shape, f32),
            pltpu.VMEM((n_gz,) + leaf_low.shape, f32),
            pltpu.VMEM((n_gz,) + parent_inv.shape, f32),
            pltpu.VMEM((2, LEAF_DEV, PIV, LANES), f32),
            pltpu.VMEM((n_gy, PIV, LANES), f32),
            pltpu.VMEM((n_gy, PIV, LANES), f32),
            pltpu.VMEM((n_gy, PIV, LANES), f32),
            pltpu.VMEM((n_gy, PIV, LANES), f32),
            pltpu.VMEM((PAR_DEV, 4 * BLK, 4 * BLK), jnp.bfloat16),
            pltpu.VMEM((PAR_DEV, 4 * BLK, 4 * BLK), jnp.bfloat16),
            pltpu.SMEM((rows,), jnp.int32),
            pltpu.SMEM((rows,), jnp.int32),
            pltpu.SMEM(update_target.shape[::-1], jnp.int32),
            dma((8,)), dma((3,)), dma((3,)),
            dma((3, NX - 1)), dma((3, NX - 1)), dma((3, NX - 1)), dma((3, NX - 1)),
            dma((2,)), dma((2, 2)), dma((2,)), dma((2, 2)), dma((2,)), dma((2, n_gy)),
        ],
        compiler_params=pltpu.CompilerParams(
            collective_id=0, has_side_effects=True, vmem_limit_bytes=61 * 2**20 + 7 * 2**17
        ),
        name="forward_solve",
    )(
        send_order.reshape(-1), recv_order.reshape(-1), update_target.T,
        right_side, leaf_inv, leaf_low, parent_inv,
    )


def solution(mesh):
    sizes = (mesh.shape["gx"], mesh.shape["gy"], mesh.shape["gz"])
    placed = (
        P(("gx", "gy"), "gz"),
        P(("gx", "gy"), None),
        P(("gx", "gy"), None),
        P("gx", None),
        P(("gx", "gy"), "gz", None),
        P(("gx", "gy"), "gz", None),
        P(("gx", "gy"), "gz", None),
    )
    return jax.shard_map(
        functools.partial(body, sizes), mesh=mesh, in_specs=placed,
        out_specs=P(("gx", "gy"), "gz"), check_vma=False,
    )
```

```python
import functools

import jax
import jax.numpy as jnp
from jax import lax
from jax.experimental import pallas as pl
from jax.experimental.pallas import tpu as pltpu
from jax.sharding import PartitionSpec as P

PIV = 256
BLK = 128
LEAF_DEV = 4
PAR_DEV = 2
OWN = PAR_DEV * 4
NX = 4
MESH = pl.DeviceIdType.MESH
Y_ORDER = (4, 3, 5, 2, 6, 1, 7)
G_FAR = (4, 5, 6, 7)
G_NEAR = (2, 3, 1)
LANES = 128


def kernel(
    n_gx, n_gy, n_gz,
    send_hbm, recv_hbm, target_hbm,
    rhs_hbm, inv_hbm, low_hbm, par_hbm,
    out,
    rhs_a, rhs_b, pack_a, pack_b, mid_a, mid_b, got_a, got_b, front_a, front_b,
    inv_all, low_all, par_all, upd, slots_a, slots_b, in_a, in_b,
    inv_hi, inv_lo, low_hi, low_lo, par_hi, par_lo, send_order, recv_order, target,
    load_sem, z_send, z_recv, x_send, x_recv, f_send, f_recv,
    y_send, y_recv, g_send, g_recv, upd_send, upd_recv,
):
    gx, gy, gz = lax.axis_index("gx"), lax.axis_index("gy"), lax.axis_index("gz")
    part = n_gx // 2
    share = rhs_a.shape[0] // (n_gx * n_gy)
    lot = n_gy * share
    z_peer = gz + 1 - 2 * lax.rem(gz, 2)
    near = gx // part
    far = 1 - near

    rhs, pack, mid = (rhs_a, rhs_b), (pack_a, pack_b), (mid_a, mid_b)
    got, front = (got_a, got_b), (front_a, front_b)
    slots, arrived = (slots_a, slots_b), (in_a, in_b)
    barrier = pltpu.get_barrier_semaphore()

    def greet(px, py, pz):
        pl.semaphore_signal(barrier, inc=1, device_id=(px, py, pz), device_id_type=MESH)

    def x_peer(k):
        return lax.rem(gz + 2 * k, n_gz)

    greet(gx, gy, z_peer)
    for step in Y_ORDER:
        greet(gx, lax.rem(gy + step, n_gy), gz)
    for turn in G_FAR + G_NEAR:
        greet(lax.bitwise_xor(gx, turn), gy, gz)
    for k in range(1, NX):
        greet(gx, gy, x_peer(k))

    loads = [
        pltpu.make_async_copy(rhs_hbm.at[:, pl.ds(0, LANES)], rhs_a, load_sem.at[0]),
        pltpu.make_async_copy(inv_hbm, inv_all.at[gz], load_sem.at[1]),
        pltpu.make_async_copy(low_hbm, low_all.at[gz], load_sem.at[2]),
        pltpu.make_async_copy(rhs_hbm.at[:, pl.ds(LANES, LANES)], rhs_b, load_sem.at[3]),
        pltpu.make_async_copy(par_hbm, par_all.at[gz], load_sem.at[4]),
        pltpu.make_async_copy(send_hbm, send_order, load_sem.at[5]),
        pltpu.make_async_copy(recv_hbm, recv_order, load_sem.at[6]),
        pltpu.make_async_copy(target_hbm, target, load_sem.at[7]),
    ]
    for n in (5, 0, 1, 2, 4, 3, 6, 7):
        loads[n].start()

    def turn_of(j):
        away = (j + 1) // 2
        return n_gy // 2 + away * (1 - 2 * lax.rem(j, 2))

    def pick_and_send_along_y(h, side, far_or_near):
        places = pl.ds(pl.multiple_of(side * part, part), part)
        own = pl.ds(pl.multiple_of(gy * share, share), share)

        @pl.loop(0, n_gy)
        def _(j):
            there = lax.rem(gy + turn_of(j), n_gy)

            @pl.loop(0, part)
            def _(i):
                place = side * part + i
                base = (place * n_gy + there) * share
                at = pl.multiple_of(there * share, share)
                for r in range(share):
                    pack[h][place, pl.ds(at + r, 1), :] = rhs[h][pl.ds(send_order[base + r], 1), :]

            @pl.when(j > 0)
            def _():
                ready = lax.rem(gy + turn_of(j - 1), n_gy)
                pltpu.make_async_remote_copy(
                    src_ref=pack[h].at[places, pl.ds(pl.multiple_of(ready * share, share), share)],
                    dst_ref=mid[h].at[places, own],
                    send_sem=y_send.at[h],
                    recv_sem=y_recv.at[h, far_or_near],
                    device_id=(gx, ready, gz),
                    device_id_type=MESH,
                ).start()

        mid[h][places, own, :] = pack[h][places, own, :]

    def pick_rows(h, side):
        @pl.loop(0, part * n_gy)
        def _(c):
            place = side * part + c // n_gy
            at = pl.multiple_of(lax.rem(c, n_gy) * share, share)
            base = place * lot + at
            for r in range(share):
                pack[h][place, pl.ds(at + r, 1), :] = rhs[h][pl.ds(send_order[base + r], 1), :]

    def send_along_y(h, side, far_or_near):
        places = pl.ds(pl.multiple_of(side * part, part), part)
        own = pl.ds(pl.multiple_of(gy * share, share), share)
        for step in Y_ORDER:
            there = lax.rem(gy + step, n_gy)
            pltpu.make_async_remote_copy(
                src_ref=pack[h].at[places, pl.ds(pl.multiple_of(there * share, share), share)],
                dst_ref=mid[h].at[places, own],
                send_sem=y_send.at[h],
                recv_sem=y_recv.at[h, far_or_near],
                device_id=(gx, there, gz),
                device_id_type=MESH,
            ).start()
        mid[h][places, own, :] = pack[h][places, own, :]

    def await_y(h, far_or_near):
        bulk(mid[h].at[pl.ds(0, part), pl.ds(0, (n_gy - 1) * share)], y_recv.at[h, far_or_near])

    def send_along_gx(h, turns, far_or_near):
        own = pl.ds(pl.multiple_of(gx * lot, lot), lot)
        for turn in turns:
            there = lax.bitwise_xor(gx, turn)
            pltpu.make_async_remote_copy(
                src_ref=mid[h].at[there],
                dst_ref=got[h].at[own],
                send_sem=g_send.at[h],
                recv_sem=g_recv.at[h, far_or_near],
                device_id=(there, gy, gz),
                device_id_type=MESH,
            ).start()

    def keep_own(h):
        got[h][pl.ds(pl.multiple_of(gx * lot, lot), lot), :] = mid[h][gx]

    def await_gx(h):
        bulk(got[h].at[pl.ds(0, len(G_FAR) * lot)], g_recv.at[h, 0])
        bulk(got[h].at[pl.ds(0, len(G_NEAR) * lot)], g_recv.at[h, 1])

    def bulk(view, sem):
        pltpu.make_async_copy(view, view, sem).wait()

    def take_rows(h):
        @pl.loop(0, front[h].shape[0] // 32)
        def _(c):
            base = pl.multiple_of(c * 32, 32)
            for r in range(32):
                front[h][pl.ds(base + r, 1), :] = got[h][pl.ds(recv_order[base + r], 1), :]

    def piece(w, place):
        if w < 2:
            return (inv_all, low_all)[w].at[place]
        return par_all.at[place, w - 2]

    def factor_copy(w, place, send_sem, recv_sem, to):
        return pltpu.make_async_remote_copy(
            src_ref=piece(w, place), dst_ref=piece(w, place), send_sem=send_sem, recv_sem=recv_sem,
            device_id=(gx, gy, to), device_id_type=MESH,
        )

    def z_copy(w):
        return factor_copy(w, gz, z_send.at[w], z_recv.at[w], z_peer)

    def x_copy(w, k):
        return factor_copy(w, gz, x_send.at[w, k - 1], x_recv.at[w, k - 1], x_peer(k))

    def f_copy(w, k):
        return factor_copy(w, z_peer, f_send.at[w, k - 1], f_recv.at[w, k - 1], x_peer(k))

    def share_along_x(w):
        for k in (1, 3, 2):
            x_copy(w, k).start()

    def forward_factor(w):
        z_copy(w).wait_recv()
        for k in (1, 3, 2):
            f_copy(w, k).start()

    def await_factor(w):
        for k in range(1, NX):
            x_copy(w, k).wait_recv()
            f_copy(w, k).wait_recv()

    def splat(leaf, j):
        return jnp.full((8, LANES), target[j, leaf], jnp.int32)

    def owned_by(first, place):
        return jnp.logical_and(first >= place * OWN, first < place * OWN + OWN)

    def keep(mask, new, old):
        shape = new.shape
        tiles = (shape[0] // 8, 8, LANES)
        mask = jnp.broadcast_to(mask[None], tiles)
        return jnp.where(mask, new.reshape(tiles), old.reshape(tiles)).reshape(shape)

    def split(x):
        high = x.astype(jnp.bfloat16)
        return high, (x - high.astype(jnp.float32)).astype(jnp.bfloat16)

    def split_factor(whole, high, low):
        rows = whole.shape[2]
        for f in range(whole.shape[1]):
            for g in range(n_gz):
                at = pl.ds(g * rows, rows)
                high[f, at, :], low[f, at, :] = split(whole[g, f])

    def product(a_high, a_low, b):
        high, low = split(b)
        both = jnp.dot(
            a_high, jnp.concatenate([high, low], axis=1), preferred_element_type=jnp.float32
        )
        rest = jnp.dot(a_low, high, preferred_element_type=jnp.float32)
        return both[:, :LANES] + both[:, LANES:] + rest

    def leaf_stage(h):
        cols = pl.ds(h * LANES, LANES)
        take_rows(h)
        for l in range(LEAF_DEV):
            rows = pl.ds(l * PIV, PIV)
            sol = product(inv_hi[l], inv_lo[l], front[h][rows, :])
            out[rows, cols] = sol
            upd[h, l] = product(low_hi[l], low_lo[l], sol)
        firsts = [splat(gy * LEAF_DEV + l, 0) for l in range(LEAF_DEV)]
        for step in Y_ORDER + (0,):
            there = lax.rem(gy + step, n_gy)
            masks = [owned_by(firsts[l], there) for l in range(1, LEAF_DEV)]
            for part in range(0, PIV, BLK):
                rows = pl.ds(part, BLK)
                chosen = upd[h, 0, rows, :]
                for l in range(1, LEAF_DEV):
                    chosen = keep(masks[l - 1], upd[h, l, rows, :], chosen)
                if step == 0:
                    arrived[h][gy, rows, :] = chosen
                else:
                    slots[h][step, rows, :] = chosen
        for step in Y_ORDER:
            pltpu.make_async_remote_copy(
                src_ref=slots[h].at[step], dst_ref=arrived[h].at[gy],
                send_sem=upd_send.at[h], recv_sem=upd_recv.at[h, step],
                device_id=(gx, lax.rem(gy + step, n_gy), gz), device_id_type=MESH,
            ).start()

    def absorb(h, source):
        zeros = jnp.zeros((BLK, LANES), jnp.float32)
        one = two = jnp.full((8, LANES), -1, jnp.int32)
        for l in range(LEAF_DEV):
            leaf = source * LEAF_DEV + l
            t_one, t_two = splat(leaf, 0), splat(leaf, 1)
            mine = owned_by(t_one, gy)
            one = jnp.where(mine, t_one, one)
            two = jnp.where(mine, t_two, two)
        for b in range(OWN):
            here = gy * OWN + b
            rows = pl.ds(LEAF_DEV * PIV + b * BLK, BLK)
            piece = keep(two == here, arrived[h][source, pl.ds(BLK, BLK), :], zeros)
            piece = keep(one == here, arrived[h][source, pl.ds(0, BLK), :], piece)
            front[h][rows, :] = front[h][rows, :] - piece

    def absorb_all(h):
        absorb(h, gy)

        @pl.loop(0, n_gy - 1)
        def _(j):
            turn = turn_of(j)
            source = lax.rem(gy + n_gy - turn, n_gy)
            pltpu.make_async_copy(
                arrived[h].at[source], arrived[h].at[source], upd_recv.at[h, turn]
            ).wait()
            absorb(h, source)

    def parent_stage(h):
        absorb_all(h)
        cols = pl.ds(h * LANES, LANES)
        for p in range(PAR_DEV):
            rows = pl.ds(LEAF_DEV * PIV + p * 4 * BLK, 4 * BLK)
            out[rows, cols] = product(par_hi[p], par_lo[p], front[h][rows, :])

    loads[1].wait()
    loads[2].wait()
    loads[4].wait()
    loads[5].wait()
    loads[0].wait()
    pl.semaphore_wait(barrier, n_gx + n_gy - 2 + NX)
    z_copy(0).start()
    z_copy(1).start()
    pick_and_send_along_y(0, far, 0)
    share_along_x(0)
    share_along_x(1)
    pick_and_send_along_y(0, near, 1)
    loads[3].wait()
    pick_rows(1, far)
    pick_rows(1, near)
    loads[6].wait()
    loads[7].wait()
    await_y(0, 0)
    send_along_gx(0, G_FAR, 0)
    send_along_y(1, far, 0)
    forward_factor(0)
    forward_factor(1)
    share_along_x(2)
    share_along_x(3)
    await_y(0, 1)
    send_along_gx(0, G_NEAR, 1)
    send_along_y(1, near, 1)
    keep_own(0)
    await_factor(0)
    split_factor(inv_all, inv_hi, inv_lo)
    await_factor(1)
    split_factor(low_all, low_hi, low_lo)
    await_gx(0)
    await_y(1, 0)
    send_along_gx(1, G_FAR, 0)
    leaf_stage(0)
    await_y(1, 1)
    send_along_gx(1, G_NEAR, 1)
    keep_own(1)
    await_gx(1)
    z_copy(2).start()
    z_copy(3).start()
    leaf_stage(1)
    forward_factor(2)
    forward_factor(3)
    await_factor(2)
    await_factor(3)
    split_factor(par_all, par_hi, par_lo)
    parent_stage(0)
    parent_stage(1)
    for w in range(4):
        z_copy(w).wait_send()
        for k in range(1, NX):
            x_copy(w, k).wait_send()
            f_copy(w, k).wait_send()
    for h in range(2):
        bulk(mid[h].at[:, pl.ds(0, (n_gy - 1) * share)], y_send.at[h])
        bulk(got[h].at[pl.ds(0, (n_gx - 1) * lot)], g_send.at[h])
        bulk(slots[h].at[pl.ds(0, n_gy - 1)], upd_send.at[h])


def body(sizes, right_side, send_order, recv_order, update_target, leaf_inv, leaf_low, parent_inv):
    n_gx, n_gy, n_gz = sizes
    rows = right_side.shape[0]
    f32 = jnp.float32
    any_space = pl.BlockSpec(memory_space=pl.ANY)
    half = pltpu.VMEM((rows, LANES), f32)
    lots = pltpu.VMEM((n_gx, rows // n_gx, LANES), f32)
    leaf_half = pltpu.VMEM((LEAF_DEV, PIV, PIV), jnp.bfloat16)
    dma = pltpu.SemaphoreType.DMA
    return pl.pallas_call(
        functools.partial(kernel, n_gx, n_gy, n_gz),
        out_shape=pltpu.VMEM(right_side.shape, f32),
        in_specs=[any_space, any_space, any_space, any_space, any_space, any_space, any_space],
        out_specs=pl.BlockSpec(memory_space=pltpu.VMEM),
        scratch_shapes=[
            half, half, lots, lots, lots, lots, half, half, half, half,
            pltpu.VMEM((n_gz,) + leaf_inv.shape, f32),
            pltpu.VMEM((n_gz,) + leaf_low.shape, f32),
            pltpu.VMEM((n_gz,) + parent_inv.shape, f32),
            pltpu.VMEM((2, LEAF_DEV, PIV, LANES), f32),
            pltpu.VMEM((n_gy, PIV, LANES), f32),
            pltpu.VMEM((n_gy, PIV, LANES), f32),
            pltpu.VMEM((n_gy, PIV, LANES), f32),
            pltpu.VMEM((n_gy, PIV, LANES), f32),
            leaf_half, leaf_half, leaf_half, leaf_half,
            pltpu.VMEM((PAR_DEV, 4 * BLK, 4 * BLK), jnp.bfloat16),
            pltpu.VMEM((PAR_DEV, 4 * BLK, 4 * BLK), jnp.bfloat16),
            pltpu.SMEM((rows,), jnp.int32),
            pltpu.SMEM((rows,), jnp.int32),
            pltpu.SMEM(update_target.shape[::-1], jnp.int32),
            dma((8,)), dma((4,)), dma((4,)),
            dma((4, NX - 1)), dma((4, NX - 1)), dma((4, NX - 1)), dma((4, NX - 1)),
            dma((2,)), dma((2, 2)), dma((2,)), dma((2, 2)), dma((2,)), dma((2, n_gy)),
        ],
        compiler_params=pltpu.CompilerParams(
            collective_id=0, has_side_effects=True, vmem_limit_bytes=61 * 2**20 + 7 * 2**17
        ),
        name="forward_solve",
    )(
        send_order.reshape(-1), recv_order.reshape(-1), update_target.T,
        right_side, leaf_inv, leaf_low, parent_inv,
    )


def solution(mesh):
    sizes = (mesh.shape["gx"], mesh.shape["gy"], mesh.shape["gz"])
    placed = (
        P(("gx", "gy"), "gz"),
        P(("gx", "gy"), None),
        P(("gx", "gy"), None),
        P("gx", None),
        P(("gx", "gy"), "gz", None),
        P(("gx", "gy"), "gz", None),
        P(("gx", "gy"), "gz", None),
    )
    return jax.shard_map(
        functools.partial(body, sizes), mesh=mesh, in_specs=placed,
        out_specs=P(("gx", "gy"), "gz"), check_vma=False,
    )
```

```python
import functools

import jax
import jax.numpy as jnp
from jax import lax
from jax.experimental import pallas as pl
from jax.experimental.pallas import tpu as pltpu
from jax.sharding import PartitionSpec as P

PIV = 256
BLK = 128
LEAF_DEV = 4
PAR_DEV = 2
OWN = PAR_DEV * 4
NX = 4
MESH = pl.DeviceIdType.MESH
Y_ORDER = (4, 3, 5, 2, 6, 1, 7)
G_FAR = (4, 5, 6, 7)
G_NEAR = (2, 3, 1)
LANES = 128


def kernel(
    n_gx, n_gy, n_gz,
    send_hbm, recv_hbm, target_hbm,
    rhs_hbm, inv_hbm, low_hbm, par_hbm,
    out,
    rhs_a, rhs_b, pack_a, pack_b, mid_a, mid_b, got_a, got_b, front_a, front_b,
    inv_all, low_all, par_all, upd, slots_a, slots_b, in_a, in_b,
    inv_hi, inv_lo, low_hi, low_lo, par_hi, par_lo, send_order, recv_order, target,
    load_sem, z_send, z_recv, x_send, x_recv, f_send, f_recv,
    y_send, y_recv, g_send, g_recv, upd_send, upd_recv,
):
    gx, gy, gz = lax.axis_index("gx"), lax.axis_index("gy"), lax.axis_index("gz")
    part = n_gx // 2
    share = rhs_a.shape[0] // (n_gx * n_gy)
    lot = n_gy * share
    z_peer = gz + 1 - 2 * lax.rem(gz, 2)
    near = gx // part
    far = 1 - near

    rhs, pack, mid = (rhs_a, rhs_b), (pack_a, pack_b), (mid_a, mid_b)
    got, front = (got_a, got_b), (front_a, front_b)
    slots, arrived = (slots_a, slots_b), (in_a, in_b)
    barrier = pltpu.get_barrier_semaphore()

    def greet(px, py, pz):
        pl.semaphore_signal(barrier, inc=1, device_id=(px, py, pz), device_id_type=MESH)

    def x_peer(k):
        return lax.rem(gz + 2 * k, n_gz)

    greet(gx, gy, z_peer)
    for step in Y_ORDER:
        greet(gx, lax.rem(gy + step, n_gy), gz)
    for turn in G_FAR + G_NEAR:
        greet(lax.bitwise_xor(gx, turn), gy, gz)
    for k in range(1, NX):
        greet(gx, gy, x_peer(k))

    loads = [
        pltpu.make_async_copy(rhs_hbm.at[:, pl.ds(0, LANES)], rhs_a, load_sem.at[0]),
        pltpu.make_async_copy(inv_hbm, inv_all.at[gz], load_sem.at[1]),
        pltpu.make_async_copy(low_hbm, low_all.at[gz], load_sem.at[2]),
        pltpu.make_async_copy(rhs_hbm.at[:, pl.ds(LANES, LANES)], rhs_b, load_sem.at[3]),
        pltpu.make_async_copy(par_hbm, par_all.at[gz], load_sem.at[4]),
        pltpu.make_async_copy(send_hbm, send_order, load_sem.at[5]),
        pltpu.make_async_copy(recv_hbm, recv_order, load_sem.at[6]),
        pltpu.make_async_copy(target_hbm, target, load_sem.at[7]),
    ]
    for n in (5, 0, 1, 2, 4, 3, 6, 7):
        loads[n].start()

    def turn_of(j):
        away = (j + 1) // 2
        return n_gy // 2 + away * (1 - 2 * lax.rem(j, 2))

    def pick_and_send_along_y(h, side, far_or_near):
        places = pl.ds(pl.multiple_of(side * part, part), part)
        own = pl.ds(pl.multiple_of(gy * share, share), share)

        @pl.loop(0, n_gy)
        def _(j):
            there = lax.rem(gy + turn_of(j), n_gy)

            @pl.loop(0, part)
            def _(i):
                place = side * part + i
                base = (place * n_gy + there) * share
                at = pl.multiple_of(there * share, share)
                for r in range(share):
                    pack[h][place, pl.ds(at + r, 1), :] = rhs[h][pl.ds(send_order[base + r], 1), :]

            @pl.when(j > 0)
            def _():
                ready = lax.rem(gy + turn_of(j - 1), n_gy)
                pltpu.make_async_remote_copy(
                    src_ref=pack[h].at[places, pl.ds(pl.multiple_of(ready * share, share), share)],
                    dst_ref=mid[h].at[places, own],
                    send_sem=y_send.at[h],
                    recv_sem=y_recv.at[h, far_or_near],
                    device_id=(gx, ready, gz),
                    device_id_type=MESH,
                ).start()

        mid[h][places, own, :] = pack[h][places, own, :]

    def pick_rows(h, side):
        @pl.loop(0, part * n_gy)
        def _(c):
            place = side * part + c // n_gy
            at = pl.multiple_of(lax.rem(c, n_gy) * share, share)
            base = place * lot + at
            for r in range(share):
                pack[h][place, pl.ds(at + r, 1), :] = rhs[h][pl.ds(send_order[base + r], 1), :]

    def send_along_y(h, side, far_or_near):
        places = pl.ds(pl.multiple_of(side * part, part), part)
        own = pl.ds(pl.multiple_of(gy * share, share), share)
        for step in Y_ORDER:
            there = lax.rem(gy + step, n_gy)
            pltpu.make_async_remote_copy(
                src_ref=pack[h].at[places, pl.ds(pl.multiple_of(there * share, share), share)],
                dst_ref=mid[h].at[places, own],
                send_sem=y_send.at[h],
                recv_sem=y_recv.at[h, far_or_near],
                device_id=(gx, there, gz),
                device_id_type=MESH,
            ).start()
        mid[h][places, own, :] = pack[h][places, own, :]

    def await_y(h, far_or_near):
        bulk(mid[h].at[pl.ds(0, part), pl.ds(0, (n_gy - 1) * share)], y_recv.at[h, far_or_near])

    def send_along_gx(h, turns, far_or_near):
        own = pl.ds(pl.multiple_of(gx * lot, lot), lot)
        for turn in turns:
            there = lax.bitwise_xor(gx, turn)
            pltpu.make_async_remote_copy(
                src_ref=mid[h].at[there],
                dst_ref=got[h].at[own],
                send_sem=g_send.at[h],
                recv_sem=g_recv.at[h, far_or_near],
                device_id=(there, gy, gz),
                device_id_type=MESH,
            ).start()

    def keep_own(h):
        got[h][pl.ds(pl.multiple_of(gx * lot, lot), lot), :] = mid[h][gx]

    def await_gx(h):
        bulk(got[h].at[pl.ds(0, len(G_FAR) * lot)], g_recv.at[h, 0])
        bulk(got[h].at[pl.ds(0, len(G_NEAR) * lot)], g_recv.at[h, 1])

    def bulk(view, sem):
        pltpu.make_async_copy(view, view, sem).wait()

    def take_rows(h, first, last):
        @pl.loop(first // 32, last // 32)
        def _(c):
            base = pl.multiple_of(c * 32, 32)
            for r in range(32):
                front[h][pl.ds(base + r, 1), :] = got[h][pl.ds(recv_order[base + r], 1), :]

    def piece(w, place):
        if w < 2:
            return (inv_all, low_all)[w].at[place]
        return par_all.at[place, w - 2]

    def factor_copy(w, place, send_sem, recv_sem, to):
        return pltpu.make_async_remote_copy(
            src_ref=piece(w, place), dst_ref=piece(w, place), send_sem=send_sem, recv_sem=recv_sem,
            device_id=(gx, gy, to), device_id_type=MESH,
        )

    def z_copy(w):
        return factor_copy(w, gz, z_send.at[w], z_recv.at[w], z_peer)

    def x_copy(w, k):
        return factor_copy(w, gz, x_send.at[w, k - 1], x_recv.at[w, k - 1], x_peer(k))

    def f_copy(w, k):
        return factor_copy(w, z_peer, f_send.at[w, k - 1], f_recv.at[w, k - 1], x_peer(k))

    def share_along_x(w):
        for k in (1, 3, 2):
            x_copy(w, k).start()

    def forward_factor(w):
        z_copy(w).wait_recv()
        for k in (1, 3, 2):
            f_copy(w, k).start()

    def await_factor(w):
        for k in range(1, NX):
            x_copy(w, k).wait_recv()
            f_copy(w, k).wait_recv()

    def splat(leaf, j):
        return jnp.full((8, LANES), target[j, leaf], jnp.int32)

    def owned_by(first, place):
        return jnp.logical_and(first >= place * OWN, first < place * OWN + OWN)

    def keep(mask, new, old):
        shape = new.shape
        tiles = (shape[0] // 8, 8, LANES)
        mask = jnp.broadcast_to(mask[None], tiles)
        return jnp.where(mask, new.reshape(tiles), old.reshape(tiles)).reshape(shape)

    def split(x):
        high = x.astype(jnp.bfloat16)
        return high, (x - high.astype(jnp.float32)).astype(jnp.bfloat16)

    def split_factor(whole, high, low):
        rows = whole.shape[2]
        for f in range(whole.shape[1]):
            for g in range(n_gz):
                at = pl.ds(g * rows, rows)
                high[f, at, :], low[f, at, :] = split(whole[g, f])

    def product(a_high, a_low, b):
        high, low = split(b)
        both = jnp.dot(
            a_high, jnp.concatenate([high, low], axis=1), preferred_element_type=jnp.float32
        )
        rest = jnp.dot(a_low, high, preferred_element_type=jnp.float32)
        return both[:, :LANES] + both[:, LANES:] + rest

    def leaf_stage(h):
        cols = pl.ds(h * LANES, LANES)
        take_rows(h, 0, LEAF_DEV * PIV)
        for l in range(LEAF_DEV):
            rows = pl.ds(l * PIV, PIV)
            sol = product(inv_hi[l], inv_lo[l], front[h][rows, :])
            out[rows, cols] = sol
            upd[h, l] = product(low_hi[l], low_lo[l], sol)
        firsts = [splat(gy * LEAF_DEV + l, 0) for l in range(LEAF_DEV)]
        for step in Y_ORDER + (0,):
            there = lax.rem(gy + step, n_gy)
            masks = [owned_by(firsts[l], there) for l in range(1, LEAF_DEV)]
            for part in range(0, PIV, BLK):
                rows = pl.ds(part, BLK)
                chosen = upd[h, 0, rows, :]
                for l in range(1, LEAF_DEV):
                    chosen = keep(masks[l - 1], upd[h, l, rows, :], chosen)
                if step == 0:
                    arrived[h][gy, rows, :] = chosen
                else:
                    slots[h][step, rows, :] = chosen
        for step in Y_ORDER:
            pltpu.make_async_remote_copy(
                src_ref=slots[h].at[step], dst_ref=arrived[h].at[gy],
                send_sem=upd_send.at[h], recv_sem=upd_recv.at[h, step],
                device_id=(gx, lax.rem(gy + step, n_gy), gz), device_id_type=MESH,
            ).start()
        take_rows(h, LEAF_DEV * PIV, front[h].shape[0])

    def absorb(h, source):
        zeros = jnp.zeros((BLK, LANES), jnp.float32)
        one = two = jnp.full((8, LANES), -1, jnp.int32)
        for l in range(LEAF_DEV):
            leaf = source * LEAF_DEV + l
            t_one, t_two = splat(leaf, 0), splat(leaf, 1)
            mine = owned_by(t_one, gy)
            one = jnp.where(mine, t_one, one)
            two = jnp.where(mine, t_two, two)
        for b in range(OWN):
            here = gy * OWN + b
            rows = pl.ds(LEAF_DEV * PIV + b * BLK, BLK)
            piece = keep(two == here, arrived[h][source, pl.ds(BLK, BLK), :], zeros)
            piece = keep(one == here, arrived[h][source, pl.ds(0, BLK), :], piece)
            front[h][rows, :] = front[h][rows, :] - piece

    def absorb_all(h):
        absorb(h, gy)

        @pl.loop(0, n_gy - 1)
        def _(j):
            turn = turn_of(j)
            source = lax.rem(gy + n_gy - turn, n_gy)
            pltpu.make_async_copy(
                arrived[h].at[source], arrived[h].at[source], upd_recv.at[h, turn]
            ).wait()
            absorb(h, source)

    def parent_stage(h):
        absorb_all(h)
        cols = pl.ds(h * LANES, LANES)
        for p in range(PAR_DEV):
            rows = pl.ds(LEAF_DEV * PIV + p * 4 * BLK, 4 * BLK)
            out[rows, cols] = product(par_hi[p], par_lo[p], front[h][rows, :])

    loads[1].wait()
    loads[2].wait()
    loads[4].wait()
    loads[5].wait()
    loads[0].wait()
    pl.semaphore_wait(barrier, n_gx + n_gy - 2 + NX)
    z_copy(0).start()
    z_copy(1).start()
    pick_and_send_along_y(0, far, 0)
    share_along_x(0)
    share_along_x(1)
    pick_and_send_along_y(0, near, 1)
    loads[3].wait()
    pick_rows(1, far)
    pick_rows(1, near)
    loads[6].wait()
    loads[7].wait()
    await_y(0, 0)
    send_along_gx(0, G_FAR, 0)
    send_along_y(1, far, 0)
    forward_factor(0)
    forward_factor(1)
    share_along_x(2)
    share_along_x(3)
    await_y(0, 1)
    send_along_gx(0, G_NEAR, 1)
    send_along_y(1, near, 1)
    keep_own(0)
    await_factor(0)
    split_factor(inv_all, inv_hi, inv_lo)
    await_factor(1)
    split_factor(low_all, low_hi, low_lo)
    await_gx(0)
    await_y(1, 0)
    send_along_gx(1, G_FAR, 0)
    leaf_stage(0)
    await_y(1, 1)
    send_along_gx(1, G_NEAR, 1)
    keep_own(1)
    await_gx(1)
    z_copy(2).start()
    z_copy(3).start()
    leaf_stage(1)
    forward_factor(2)
    forward_factor(3)
    await_factor(2)
    await_factor(3)
    split_factor(par_all, par_hi, par_lo)
    parent_stage(0)
    parent_stage(1)
    for w in range(4):
        z_copy(w).wait_send()
        for k in range(1, NX):
            x_copy(w, k).wait_send()
            f_copy(w, k).wait_send()
    for h in range(2):
        bulk(mid[h].at[:, pl.ds(0, (n_gy - 1) * share)], y_send.at[h])
        bulk(got[h].at[pl.ds(0, (n_gx - 1) * lot)], g_send.at[h])
        bulk(slots[h].at[pl.ds(0, n_gy - 1)], upd_send.at[h])


def body(sizes, right_side, send_order, recv_order, update_target, leaf_inv, leaf_low, parent_inv):
    n_gx, n_gy, n_gz = sizes
    rows = right_side.shape[0]
    f32 = jnp.float32
    any_space = pl.BlockSpec(memory_space=pl.ANY)
    half = pltpu.VMEM((rows, LANES), f32)
    lots = pltpu.VMEM((n_gx, rows // n_gx, LANES), f32)
    leaf_half = pltpu.VMEM((LEAF_DEV, PIV, PIV), jnp.bfloat16)
    dma = pltpu.SemaphoreType.DMA
    return pl.pallas_call(
        functools.partial(kernel, n_gx, n_gy, n_gz),
        out_shape=pltpu.VMEM(right_side.shape, f32),
        in_specs=[any_space, any_space, any_space, any_space, any_space, any_space, any_space],
        out_specs=pl.BlockSpec(memory_space=pltpu.VMEM),
        scratch_shapes=[
            half, half, lots, lots, lots, lots, half, half, half, half,
            pltpu.VMEM((n_gz,) + leaf_inv.shape, f32),
            pltpu.VMEM((n_gz,) + leaf_low.shape, f32),
            pltpu.VMEM((n_gz,) + parent_inv.shape, f32),
            pltpu.VMEM((2, LEAF_DEV, PIV, LANES), f32),
            pltpu.VMEM((n_gy, PIV, LANES), f32),
            pltpu.VMEM((n_gy, PIV, LANES), f32),
            pltpu.VMEM((n_gy, PIV, LANES), f32),
            pltpu.VMEM((n_gy, PIV, LANES), f32),
            leaf_half, leaf_half, leaf_half, leaf_half,
            pltpu.VMEM((PAR_DEV, 4 * BLK, 4 * BLK), jnp.bfloat16),
            pltpu.VMEM((PAR_DEV, 4 * BLK, 4 * BLK), jnp.bfloat16),
            pltpu.SMEM((rows,), jnp.int32),
            pltpu.SMEM((rows,), jnp.int32),
            pltpu.SMEM(update_target.shape[::-1], jnp.int32),
            dma((8,)), dma((4,)), dma((4,)),
            dma((4, NX - 1)), dma((4, NX - 1)), dma((4, NX - 1)), dma((4, NX - 1)),
            dma((2,)), dma((2, 2)), dma((2,)), dma((2, 2)), dma((2,)), dma((2, n_gy)),
        ],
        compiler_params=pltpu.CompilerParams(
            collective_id=0, has_side_effects=True, vmem_limit_bytes=61 * 2**20 + 7 * 2**17
        ),
        name="forward_solve",
    )(
        send_order.reshape(-1), recv_order.reshape(-1), update_target.T,
        right_side, leaf_inv, leaf_low, parent_inv,
    )


def solution(mesh):
    sizes = (mesh.shape["gx"], mesh.shape["gy"], mesh.shape["gz"])
    placed = (
        P(("gx", "gy"), "gz"),
        P(("gx", "gy"), None),
        P(("gx", "gy"), None),
        P("gx", None),
        P(("gx", "gy"), "gz", None),
        P(("gx", "gy"), "gz", None),
        P(("gx", "gy"), "gz", None),
    )
    return jax.shard_map(
        functools.partial(body, sizes), mesh=mesh, in_specs=placed,
        out_specs=P(("gx", "gy"), "gz"), check_vma=False,
    )
```
